16 devices in a mesh: dp: 2 (over y, z), tp: 8 (over x, core).
Axes of the slice: x: 4, y: 2, z: 1, core: 2. Of those that a mesh axis runs over, the one named last changes fastest.
The devices are a block of a 4x4x8 slice.
Arguments:
- x_in: bfloat16 [256, 4096], P('dp'), parts along dimension 0
- seq_lens: int32 [256], P('dp'), parts along dimension 0
- g_attn: bfloat16 [2, 4096], replicated
- g_mlp: bfloat16 [2, 4096], replicated
- w_q: bfloat16 [2, 4096, 4096], P(None, None, 'tp')
- b_q: bfloat16 [2, 4096], P(None, 'tp')
- w_k: bfloat16 [2, 4096, 1024], P(None, None, 'tp')
- b_k: bfloat16 [2, 1024], P(None, 'tp')
- w_v: bfloat16 [2, 4096, 1024], P(None, None, 'tp')
- b_v: bfloat16 [2, 1024], P(None, 'tp')
- w_o: bfloat16 [2, 4096, 4096], P(None, 'tp')
- w_gate: bfloat16 [2, 4096, 12288], P(None, None, 'tp')
- w_up: bfloat16 [2, 4096, 12288], P(None, None, 'tp')
- w_down: bfloat16 [2, 12288, 4096], P(None, 'tp')
- k_cache: bfloat16 [2, 256, 128, 8, 128], P(None, 'dp', None, 'tp'), parts along dimension 1
- v_cache: bfloat16 [2, 256, 128, 8, 128], P(None, 'dp', None, 'tp'), parts along dimension 1
Outputs:
- output 1: bfloat16 [256, 4096], P('dp'), parts along dimension 0
- output 2: bfloat16 [2, 256, 128, 8, 128], P(None, 'dp', None, 'tp'), parts along dimension 1
- output 3: bfloat16 [2, 256, 128, 8, 128], P(None, 'dp', None, 'tp'), parts along dimension 1
There are 2 independent parts. The reference program is written for one: setup_inputs(seed, part) draws one part's arguments, and reference() takes and returns one part's arrays. A program takes and returns all parts, laid end to end along the dimension named above; an argument that names none is the same for every part.
All inputs are finite; a program needn't handle non-finite values.
Results may differ from the reference program's by a relative error of at most 0.02.
Values are sent between devices in bfloat16 or wider.
A program may use at most 768 MiB of HBM per device.

```python
import math
import jax
import jax.numpy as jnp
from jax import lax

D = 4096
HEADS = 32
KV_HEADS = 8
HEAD = 128
FF = 12288
BATCH = 128
CACHE = 128
LAYERS = 2
ROPE_THETA = 1000000.0
EPS = 1e-6


def setup_inputs(seed: int = 0, part: int = 0) -> dict:
    root_key = jax.random.key(seed)
    weight_keys = jax.random.split(root_key, 12)
    part_keys = jax.random.split(jax.random.fold_in(root_key, part), 5)
    group_size = HEADS // KV_HEADS
    q_width = HEADS * HEAD
    kv_width = KV_HEADS * HEAD
    couple = 0.6 * math.log(CACHE) / math.sqrt(HEAD)

    def normal(sub_key, arr_shape, arr_scale):
        return jax.random.normal(sub_key, arr_shape, jnp.float32) * arr_scale

    seq_lens = jax.random.randint(part_keys[1], (BATCH,), CACHE // 16, CACHE, dtype=jnp.int32)
    seq_lens = seq_lens.at[0].set(CACHE - 1).at[1].set(CACHE // 16)
    k_bias = normal(weight_keys[5], (LAYERS, KV_HEADS, 1, HEAD), 1.0)
    q_bias = couple * k_bias + normal(weight_keys[3], (LAYERS, KV_HEADS, group_size, HEAD), 1.0)
    cache_shape = (LAYERS, BATCH, CACHE, KV_HEADS, HEAD)
    v_mean = normal(part_keys[3], (LAYERS, BATCH, 1, KV_HEADS, HEAD), 1.0)
    return {
        "x_in": normal(part_keys[0], (BATCH, D), 1.0).astype(jnp.bfloat16),
        "seq_lens": seq_lens,
        "g_attn": (1.0 + normal(weight_keys[0], (LAYERS, D), 0.25)).astype(jnp.bfloat16),
        "g_mlp": (1.0 + normal(weight_keys[1], (LAYERS, D), 0.25)).astype(jnp.bfloat16),
        "w_q": normal(weight_keys[2], (LAYERS, D, q_width), D ** -0.5).astype(jnp.bfloat16),
        "b_q": q_bias.reshape(LAYERS, q_width).astype(jnp.bfloat16),
        "w_k": normal(weight_keys[4], (LAYERS, D, kv_width), D ** -0.5).astype(jnp.bfloat16),
        "b_k": k_bias.reshape(LAYERS, kv_width).astype(jnp.bfloat16),
        "w_v": normal(weight_keys[6], (LAYERS, D, kv_width), D ** -0.5).astype(jnp.bfloat16),
        "b_v": normal(weight_keys[7], (LAYERS, kv_width), 1.0).astype(jnp.bfloat16),
        "w_o": normal(weight_keys[8], (LAYERS, q_width, D), q_width ** -0.5).astype(jnp.bfloat16),
        "w_gate": normal(weight_keys[9], (LAYERS, D, FF), D ** -0.5).astype(jnp.bfloat16),
        "w_up": normal(weight_keys[10], (LAYERS, D, FF), D ** -0.5).astype(jnp.bfloat16),
        "w_down": normal(weight_keys[11], (LAYERS, FF, D), FF ** -0.5).astype(jnp.bfloat16),
        "k_cache": normal(part_keys[2], cache_shape, 1.0).astype(jnp.bfloat16),
        "v_cache": (v_mean + normal(part_keys[4], cache_shape, 1.0)).astype(jnp.bfloat16),
    }


def rms_norm(vec_in, gain_vec):
    vec_f32 = vec_in.astype(jnp.float32)
    mean_sq = jnp.mean(vec_f32 * vec_f32, axis=-1, keepdims=True)
    return (vec_f32 * lax.rsqrt(mean_sq + EPS) * gain_vec.astype(jnp.float32)).astype(jnp.bfloat16)


def rope_tables(seq_lens, head_dim):
    half_dim = head_dim // 2
    inv_freq = ROPE_THETA ** (-2.0 * jnp.arange(half_dim, dtype=jnp.float32) / head_dim)
    angles = seq_lens.astype(jnp.float32)[:, None] * inv_freq[None, :]
    angles = jnp.concatenate([angles, angles], axis=-1)[:, None, :]
    return jnp.cos(angles), jnp.sin(angles)


def apply_rope(vec_in, cos_tab, sin_tab):
    half_dim = vec_in.shape[-1] // 2
    rotated = jnp.concatenate([-vec_in[..., half_dim:], vec_in[..., :half_dim]], axis=-1)
    return vec_in * cos_tab + rotated * sin_tab


def decoder_layer(x_in, seq_lens, cos_tab, sin_tab, params):
    g_attn, g_mlp, w_q, b_q, w_k, b_k, w_v, b_v, w_o, w_gate, w_up, w_down, k_cache, v_cache = params
    num_rows = x_in.shape[0]
    group_size = HEADS // KV_HEADS
    normed = rms_norm(x_in, g_attn)
    q_full = jnp.dot(normed, w_q, preferred_element_type=jnp.float32) + b_q.astype(jnp.float32)
    q_rot = apply_rope(q_full.reshape(num_rows, HEADS, HEAD), cos_tab, sin_tab).astype(jnp.bfloat16)
    k_full = jnp.dot(normed, w_k, preferred_element_type=jnp.float32) + b_k.astype(jnp.float32)
    k_rot = apply_rope(k_full.reshape(num_rows, KV_HEADS, HEAD), cos_tab, sin_tab).astype(jnp.bfloat16)
    v_full = jnp.dot(normed, w_v, preferred_element_type=jnp.float32) + b_v.astype(jnp.float32)
    v_new = v_full.astype(jnp.bfloat16).reshape(num_rows, KV_HEADS, HEAD)
    slot_ids = jnp.arange(CACHE, dtype=jnp.int32)
    is_new = (slot_ids[None, :] == seq_lens[:, None])[:, :, None, None]
    k_next = jnp.where(is_new, k_rot[:, None], k_cache)
    v_next = jnp.where(is_new, v_new[:, None], v_cache)
    q_grouped = q_rot.reshape(num_rows, KV_HEADS, group_size, HEAD)

    def attend_row(row_args):
        q_row, k_row, v_row, row_len = row_args
        scores = jnp.einsum("kgd,skd->kgs", q_row.astype(jnp.float32), k_row.astype(jnp.float32)) * (HEAD ** -0.5)
        visible = slot_ids <= row_len
        scores = jnp.where(visible[None, None, :], scores, -1e30)
        attn_probs = jax.nn.softmax(scores, axis=-1).astype(jnp.bfloat16)
        out_row = jnp.einsum("kgs,skd->kgd", attn_probs.astype(jnp.float32), v_row.astype(jnp.float32))
        return out_row.astype(jnp.bfloat16)

    attn_out = lax.map(attend_row, (q_grouped, k_next, v_next, seq_lens)).reshape(num_rows, HEADS * HEAD)
    x_mid = (x_in.astype(jnp.float32) + jnp.dot(attn_out, w_o, preferred_element_type=jnp.float32)).astype(jnp.bfloat16)
    normed_mlp = rms_norm(x_mid, g_mlp)
    gate_proj = jnp.dot(normed_mlp, w_gate, preferred_element_type=jnp.float32)
    up_proj = jnp.dot(normed_mlp, w_up, preferred_element_type=jnp.float32)
    hidden_act = (jax.nn.silu(gate_proj) * up_proj).astype(jnp.bfloat16)
    x_next = (x_mid.astype(jnp.float32) + jnp.dot(hidden_act, w_down, preferred_element_type=jnp.float32)).astype(jnp.bfloat16)
    return x_next, k_next, v_next


def reference(x_in, seq_lens, g_attn, g_mlp, w_q, b_q, w_k, b_k, w_v, b_v, w_o, w_gate, w_up, w_down, k_cache, v_cache):
    cos_tab, sin_tab = rope_tables(seq_lens, HEAD)

    def layer_step(x_carry, params):
        x_next, k_next, v_next = decoder_layer(x_carry, seq_lens, cos_tab, sin_tab, params)
        return x_next, (k_next, v_next)

    layer_params = (g_attn, g_mlp, w_q, b_q, w_k, b_k, w_v, b_v, w_o, w_gate, w_up, w_down, k_cache, v_cache)
    x_out, cache_pair = lax.scan(layer_step, x_in, layer_params)
    return x_out, cache_pair[0], cache_pair[1]
```

```python
import functools
import math

import jax
import jax.numpy as jnp
from jax import lax
from jax.experimental import pallas as pl
from jax.experimental.pallas import tpu as pltpu
from jax.sharding import PartitionSpec as P

ROPE_THETA = 1000000.0
EPS = 1e-6
MESH = pl.DeviceIdType.MESH
BF16 = jnp.bfloat16
F32 = jnp.float32
NCHUNK = 4
SEQ_BLOCK = 16
HBM = pl.BlockSpec(memory_space=pltpu.HBM)
VMEM = pl.BlockSpec(memory_space=pltpu.VMEM)
SMEM = pl.BlockSpec(memory_space=pltpu.SMEM)


def attention_kernel(layer, first, seq_ref, act_ref, g_ref, bq_ref, bk_ref, bv_ref, cos_in, sin_in, wq, wk, wv, kc, vc,
                     *rest):
    rest = list(rest)
    if not first:
        rest = rest[2:]
    attn_ref, cos_ref, sin_ref, k_out, v_out = rest[:5]
    h_s, w_s, kbuf, vbuf, qs, os, kn, vn, wsem, csem, osem = rest[5:]
    rows, width = act_ref.shape
    q_width = wq.shape[2]
    head = wk.shape[2]
    slots = kbuf.shape[1]
    heads = q_width // head
    kw = width // NCHUNK
    nblk = rows // SEQ_BLOCK

    def w_copies(c):
        ks = pl.ds(c * kw, kw)
        return [
            pltpu.make_async_copy(wq.at[layer, ks, :], w_s.at[ks, pl.ds(0, q_width)], wsem.at[c, 0]),
            pltpu.make_async_copy(wk.at[layer, ks, :], w_s.at[ks, pl.ds(q_width, head)], wsem.at[c, 1]),
            pltpu.make_async_copy(wv.at[layer, ks, :], w_s.at[ks, pl.ds(q_width + head, head)], wsem.at[c, 2]),
        ]

    def c_copies(i):
        bs = pl.ds(i * SEQ_BLOCK, SEQ_BLOCK)
        return [
            pltpu.make_async_copy(kc.at[layer, bs], kbuf.at[bs], csem.at[i, 0]),
            pltpu.make_async_copy(vc.at[layer, bs], vbuf.at[bs], csem.at[i, 1]),
        ]

    def o_copies(i):
        bs = pl.ds(i * SEQ_BLOCK, SEQ_BLOCK)
        return [
            pltpu.make_async_copy(kbuf.at[bs], k_out.at[layer, bs], osem.at[i, 0]),
            pltpu.make_async_copy(vbuf.at[bs], v_out.at[layer, bs], osem.at[i, 1]),
        ]

    for c in range(NCHUNK):
        for cp in w_copies(c):
            cp.start()
    for i in range(nblk):
        for cp in c_copies(i):
            cp.start()

    if first:
        def pos_row(b, carry):
            kn[pl.ds(b, 1), :] = jnp.full((1, head), seq_ref[b].astype(F32))
            return carry
        lax.fori_loop(0, rows, pos_row, 0, unroll=8)
        lane = lax.broadcasted_iota(jnp.int32, (rows, head), 1)
        half = head // 2
        freq = (lane % half).astype(F32)
        inv_freq = jnp.exp(freq[:8] * (-2.0 / head * math.log(ROPE_THETA)))
        angle = kn[...] * jnp.broadcast_to(inv_freq[:1], (rows, head))
        cos_ref[...] = jnp.cos(angle)
        sin_ref[...] = jnp.where(lane < half, -1.0, 1.0) * jnp.sin(angle)

        def norm_block(i, carry):
            rs = pl.ds(pl.multiple_of(i * 16, 16), 16)
            xv = act_ref[rs, :].astype(F32)
            ms = jnp.mean(xv * xv, axis=-1, keepdims=True)
            gain = g_ref[...].astype(F32)[layer:layer + 1, :]
            h_s[rs, :] = (xv * lax.rsqrt(ms + EPS) * gain).astype(BF16)
            return carry
        lax.fori_loop(0, rows // 16, norm_block, 0)
        h_src = h_s
    else:
        cos_ref[...] = cos_in[...]
        sin_ref[...] = sin_in[...]
        h_src = act_ref

    acc = None
    for c in range(NCHUNK):
        for cp in w_copies(c):
            cp.wait()
        part = jnp.dot(h_src[:, c * kw:(c + 1) * kw], w_s[c * kw:(c + 1) * kw, :], preferred_element_type=F32)
        acc = part if acc is None else acc + part
    cos_t = cos_ref[...]
    sin_t = sin_ref[...]

    def rope(vec):
        return vec * cos_t + pltpu.roll(vec, head // 2, 1) * sin_t

    bq = bq_ref[...].astype(F32)[layer:layer + 1, :]
    bk = bk_ref[...].astype(F32)[layer:layer + 1, :]
    bv = bv_ref[...].astype(F32)[layer:layer + 1, :]
    for j in range(heads):
        cols = slice(j * head, (j + 1) * head)
        qs[pl.ds(j, rows, stride=8), :] = rope(acc[:, cols] + bq[:, cols])
    kn[...] = rope(acc[:, q_width:q_width + head] + bk)
    vn[...] = acc[:, q_width + head:] + bv

    scale = head ** -0.5

    def block(i, carry):
        b0 = i * SEQ_BLOCK
        for cp in c_copies(i):
            cp.wait()
        slot = lax.broadcasted_iota(jnp.int32, (slots, head), 0)
        lane = lax.broadcasted_iota(jnp.int32, (8, slots), 1)
        for j in range(SEQ_BLOCK):
            b = b0 + j
            pos = seq_ref[b]
            is_new = slot == pos
            k_b = jnp.where(is_new, jnp.broadcast_to(kn[pl.ds(b, 1), :], (slots, head)), kbuf[b].astype(F32)).astype(BF16)
            v_b = jnp.where(is_new, jnp.broadcast_to(vn[pl.ds(b, 1), :], (slots, head)), vbuf[b].astype(F32)).astype(BF16)
            kbuf[b] = k_b
            vbuf[b] = v_b
            q_b = qs[pl.ds(pl.multiple_of(b * 8, 8), 8), :].astype(BF16)
            sc = lax.dot_general(q_b, k_b, (((1,), (1,)), ((), ())), preferred_element_type=F32) * scale
            sc = jnp.where(lane <= pos, sc, -1e30)
            e = jnp.exp(sc - jnp.max(sc, axis=-1, keepdims=True))
            pr = (e / jnp.sum(e, axis=-1, keepdims=True)).astype(BF16)
            os[pl.ds(pl.multiple_of(b * 8, 8), 8), :] = jnp.dot(pr, v_b, preferred_element_type=F32)
        for cp in o_copies(i):
            cp.start()
        return carry

    lax.fori_loop(0, nblk, block, 0)
    for j in range(heads):
        attn_ref[:, j * head:(j + 1) * head] = os[pl.ds(j, rows, stride=8), :].astype(BF16)
    for i in range(nblk):
        for cp in o_copies(i):
            cp.wait()


def attention_call(layer, seq_lens, act, g_attn, b_q, b_k, b_v, cos_t, sin_t, w_q, w_k, w_v, kc, vc, outs):
    first = outs is None
    rows, width = act.shape
    head = w_k.shape[2]
    q_width = w_q.shape[2]
    slots = kc.shape[2]
    nblk = rows // SEQ_BLOCK
    table = jax.ShapeDtypeStruct((rows, head), F32)
    operands = [seq_lens, act, g_attn, b_q, b_k, b_v, cos_t, sin_t, w_q, w_k, w_v, kc, vc]
    in_specs = [SMEM, VMEM, VMEM, VMEM, VMEM, VMEM, VMEM, VMEM, HBM, HBM, HBM, HBM, HBM]
    aliases = {}
    if not first:
        aliases = {len(operands): 3, len(operands) + 1: 4}
        operands += list(outs)
        in_specs += [HBM, HBM]
    return pl.pallas_call(
        functools.partial(attention_kernel, layer, first),
        out_shape=(jax.ShapeDtypeStruct((rows, q_width), BF16), table, table,
                   jax.ShapeDtypeStruct(kc.shape, BF16), jax.ShapeDtypeStruct(vc.shape, BF16)),
        in_specs=in_specs,
        out_specs=(VMEM, VMEM, VMEM, HBM, HBM),
        scratch_shapes=[
            pltpu.VMEM((rows, width), BF16),
            pltpu.VMEM((width, q_width + 2 * head), BF16),
            pltpu.VMEM((rows, slots, head), BF16),
            pltpu.VMEM((rows, slots, head), BF16),
            pltpu.VMEM((rows * 8, head), F32),
            pltpu.VMEM((rows * 8, head), F32),
            pltpu.VMEM((rows, head), F32),
            pltpu.VMEM((rows, head), F32),
            pltpu.SemaphoreType.DMA((NCHUNK, 3)),
            pltpu.SemaphoreType.DMA((nblk, 2)),
            pltpu.SemaphoreType.DMA((nblk, 2)),
        ],
        input_output_aliases=aliases,
        compiler_params=pltpu.CompilerParams(vmem_limit_bytes=62 << 20),
        name=f"attention_{layer}",
    )(*operands)


def mlp_kernel(layer, last, attn_ref, x_ref, gm_ref, gn_ref, wo, wg, wu, wd, *rest):
    n_out = 1 if last else 2
    outs = rest[:n_out]
    (wo_s, wg_s, wu_s, wd_s, part, r0, sa, sk, r1, sb, r2, xs, hbuf, gacc, uacc, act,
     wsem, xsem, ssem, rsem) = rest[n_out:]
    rows, width = hbuf.shape[1:]
    cw = width // NCHUNK
    unit = rows // 8
    me = lax.axis_index("tp")
    core = me % 2
    chip = me // 2
    flip_near = chip + 1 - 2 * (chip % 2)
    flip_far = 3 - chip
    bit_near = ((chip + 1) // 2) % 2
    bit_far = chip // 2
    dev_p = chip * 2 + 1 - core
    dev_a = ((1 - core) * flip_near + core * flip_far) * 2 + core
    dev_b = ((1 - core) * flip_far + core * flip_near) * 2 + core
    bit_a = (1 - core) * bit_near + core * bit_far
    bit_b = (1 - core) * bit_far + core * bit_near

    def row0(core_, a_, b_):
        return pl.multiple_of((core_ * 4 + a_ * 2 + b_) * unit, unit)

    own = row0(core, bit_a, bit_b)

    def wo_copy(c):
        return pltpu.make_async_copy(wo.at[layer, :, pl.ds(c * cw, cw)], wo_s.at[:, pl.ds(c * cw, cw)], wsem.at[0, c])

    def wg_copy(c):
        return pltpu.make_async_copy(wg.at[layer, pl.ds(c * cw, cw), :], wg_s.at[pl.ds(c * cw, cw), :], wsem.at[1, c])

    def wu_copy(c):
        return pltpu.make_async_copy(wu.at[layer, pl.ds(c * cw, cw), :], wu_s.at[pl.ds(c * cw, cw), :], wsem.at[2, c])

    def wd_copy(c):
        return pltpu.make_async_copy(wd.at[layer, :, pl.ds(c * cw, cw)], wd_s.at[:, pl.ds(c * cw, cw)], wsem.at[3, c])

    for c in range(NCHUNK):
        wo_copy(c).start()
    x_copy = None
    if x_ref.shape[0] != unit:
        x_copy = pltpu.make_async_copy(x_ref.at[pl.ds(own, unit), :], xs, xsem)
        x_copy.start()
    else:
        xs[...] = x_ref[...]

    barrier = pltpu.get_barrier_semaphore()
    for dev in (dev_p, dev_a, dev_b):
        pl.semaphore_signal(barrier, inc=1, device_id={"tp": dev}, device_id_type=MESH)
    pl.semaphore_wait(barrier, 3)

    def rcopy(ar, c, k, src, dst, dev):
        return pltpu.make_async_remote_copy(
            src_ref=src, dst_ref=dst, send_sem=ssem.at[ar, c, k], recv_sem=rsem.at[ar, c, k],
            device_id={"tp": dev}, device_id_type=MESH)

    def rs_p(ar, c):
        src = part.at[ar, c, pl.ds(pl.multiple_of((1 - core) * 4 * unit, unit), 4 * unit), :]
        return rcopy(ar, c, 0, src, r0.at[ar, c], dev_p)

    def rs_a(ar, c, k):
        return rcopy(ar, c, 1 + k, sa.at[ar, c, k], r1.at[ar, c, k], dev_a)

    def rs_b(ar, c):
        return rcopy(ar, c, 3, sb.at[ar, c], r2.at[ar, c], dev_b)

    def ag(ar, c, k, start, dev):
        blk = hbuf.at[ar, pl.ds(start, unit), pl.ds(c * cw, cw)]
        return rcopy(ar, c, 4 + k, blk, blk, dev)

    blk_b = row0(core, bit_a, 1 - bit_b)
    blk_a0 = row0(core, 1 - bit_a, bit_b)
    blk_a1 = row0(core, 1 - bit_a, 1 - bit_b)

    def ag_b(ar, c):
        return ag(ar, c, 0, own, dev_b)

    def ag_a(ar, c, k):
        return ag(ar, c, 1 + k, (own, blk_b)[k], dev_a)

    def ag_p(ar, c, k):
        return ag(ar, c, 3 + k, (own, blk_b, blk_a0, blk_a1)[k], dev_p)

    def reduce_scatter(ar, make_part):
        for c in range(NCHUNK):
            part[ar, c] = make_part(c).astype(BF16)
            rs_p(ar, c).start()
        for c in range(NCHUNK):
            rs_p(ar, c).wait_recv()

            def chip_sum(a_, b_):
                mine = part[ar, c, pl.ds(row0(core, a_, b_), unit), :].astype(F32)
                theirs = r0[ar, c, pl.ds(row0(0, a_, b_), unit), :].astype(F32)
                return mine + theirs

            sa[ar, c, 0] = chip_sum(1 - bit_a, 1 - bit_b).astype(BF16)
            rs_a(ar, c, 0).start()
            sa[ar, c, 1] = chip_sum(1 - bit_a, bit_b).astype(BF16)
            sk[c, 0] = chip_sum(bit_a, 1 - bit_b)
            sk[c, 1] = chip_sum(bit_a, bit_b)
        for c in range(NCHUNK):
            rs_a(ar, c, 1).start()
        for c in range(NCHUNK):
            rs_a(ar, c, 0).wait_recv()
            sb[ar, c] = (sk[c, 0] + r1[ar, c, 0].astype(F32)).astype(BF16)
            rs_b(ar, c).start()
        for c in range(NCHUNK):
            rs_a(ar, c, 1).wait_recv()
            rs_b(ar, c).wait_recv()
            delta = sk[c, 1] + r1[ar, c, 1].astype(F32) + r2[ar, c].astype(F32)
            cols = slice(c * cw, (c + 1) * cw)
            xs[:, cols] = (xs[:, cols].astype(F32) + delta).astype(BF16)

    def gather_start(ar):
        for c in range(NCHUNK):
            ag_b(ar, c).start()
            ag_a(ar, c, 0).start()
            ag_p(ar, c, 0).start()
        for c in range(NCHUNK):
            ag_b(ar, c).wait_recv()
            ag_a(ar, c, 1).start()
            ag_p(ar, c, 1).start()
        for c in range(NCHUNK):
            ag_a(ar, c, 0).wait_recv()
            ag_p(ar, c, 2).start()
        for c in range(NCHUNK):
            ag_a(ar, c, 1).wait_recv()
            ag_p(ar, c, 3).start()

    def gather_wait(ar, c):
        for k in range(4):
            ag_p(ar, c, k).wait_recv()

    def norm_own(gain):
        xv = xs[...].astype(F32)
        ms = jnp.mean(xv * xv, axis=-1, keepdims=True)
        return (xv * lax.rsqrt(ms + EPS) * gain).astype(BF16)

    def wo_part(c):
        wo_copy(c).wait()
        if c == NCHUNK - 1:
            for i in range(NCHUNK):
                wg_copy(i).start()
                wu_copy(i).start()
            for i in range(NCHUNK):
                wd_copy(i).start()
        return jnp.dot(attn_ref[...], wo_s[:, c * cw:(c + 1) * cw], preferred_element_type=F32)

    if x_copy is not None:
        x_copy.wait()
    reduce_scatter(0, wo_part)
    hbuf[0, pl.ds(own, unit), :] = norm_own(gm_ref[...].astype(F32)[layer:layer + 1, :])
    gather_start(0)
    for c in range(NCHUNK):
        gather_wait(0, c)
        wg_copy(c).wait()
        wu_copy(c).wait()
        ks = slice(c * cw, (c + 1) * cw)
        hc = hbuf[0, :, ks]
        gp = jnp.dot(hc, wg_s[ks, :], preferred_element_type=F32)
        up = jnp.dot(hc, wu_s[ks, :], preferred_element_type=F32)
        if c == 0:
            gacc[...] = gp
            uacc[...] = up
        elif c < NCHUNK - 1:
            gacc[...] += gp
            uacc[...] += up
        else:
            gate = gacc[...] + gp
            act[...] = (gate * jax.nn.sigmoid(gate) * (uacc[...] + up)).astype(BF16)

    def wd_part(c):
        wd_copy(c).wait()
        return jnp.dot(act[...], wd_s[:, c * cw:(c + 1) * cw], preferred_element_type=F32)

    reduce_scatter(1, wd_part)
    if last:
        hbuf[1, pl.ds(own, unit), :] = xs[...]
    else:
        hbuf[1, pl.ds(own, unit), :] = norm_own(gn_ref[...].astype(F32)[layer + 1:layer + 2, :])
        outs[1][...] = xs[...]
    gather_start(1)
    for c in range(NCHUNK):
        gather_wait(1, c)
        outs[0][:, c * cw:(c + 1) * cw] = hbuf[1, :, c * cw:(c + 1) * cw]
    for ar in range(2):
        for c in range(NCHUNK):
            rs_p(ar, c).wait_send()
            rs_b(ar, c).wait_send()
            ag_b(ar, c).wait_send()
            for k in range(2):
                rs_a(ar, c, k).wait_send()
                ag_a(ar, c, k).wait_send()
            for k in range(4):
                ag_p(ar, c, k).wait_send()


def mlp_call(layer, last, attn, x_res, g_mlp, g_attn, w_o, w_gate, w_up, w_down):
    rows = attn.shape[0]
    width = w_o.shape[2]
    inner = w_o.shape[1]
    ff = w_gate.shape[2]
    unit = rows // 8
    cw = width // NCHUNK
    full = jax.ShapeDtypeStruct((rows, width), BF16)
    out_shape = (full,) if last else (full, jax.ShapeDtypeStruct((unit, width), BF16))
    x_spec = VMEM if x_res.shape[0] == unit else HBM
    return pl.pallas_call(
        functools.partial(mlp_kernel, layer, last),
        out_shape=out_shape,
        in_specs=[VMEM, x_spec, VMEM, VMEM, HBM, HBM, HBM, HBM],
        out_specs=(VMEM,) * len(out_shape),
        scratch_shapes=[
            pltpu.VMEM((inner, width), BF16),
            pltpu.VMEM((width, ff), BF16),
            pltpu.VMEM((width, ff), BF16),
            pltpu.VMEM((ff, width), BF16),
            pltpu.VMEM((2, NCHUNK, rows, cw), BF16),
            pltpu.VMEM((2, NCHUNK, rows // 2, cw), BF16),
            pltpu.VMEM((2, NCHUNK, 2, unit, cw), BF16),
            pltpu.VMEM((NCHUNK, 2, unit, cw), F32),
            pltpu.VMEM((2, NCHUNK, 2, unit, cw), BF16),
            pltpu.VMEM((2, NCHUNK, unit, cw), BF16),
            pltpu.VMEM((2, NCHUNK, unit, cw), BF16),
            pltpu.VMEM((unit, width), BF16),
            pltpu.VMEM((2, rows, width), BF16),
            pltpu.VMEM((rows, ff), F32),
            pltpu.VMEM((rows, ff), F32),
            pltpu.VMEM((rows, ff), BF16),
            pltpu.SemaphoreType.DMA((4, NCHUNK)),
            pltpu.SemaphoreType.DMA,
            pltpu.SemaphoreType.DMA((2, NCHUNK, 11)),
            pltpu.SemaphoreType.DMA((2, NCHUNK, 11)),
        ],
        compiler_params=pltpu.CompilerParams(
            vmem_limit_bytes=62 << 20, collective_id=layer, has_side_effects=True),
        name=f"mlp_{layer}",
    )(attn, x_res, g_mlp, g_attn, w_o, w_gate, w_up, w_down)


def solution(mesh):
    assert mesh.shape["tp"] == 8
    weight_col = P(None, None, "tp")
    weight_row = P(None, "tp", None)
    bias_col = P(None, "tp")
    cache_spec = P(None, "dp", None, "tp", None)
    in_specs = (P("dp", None), P("dp"), P(None, None), P(None, None), weight_col, bias_col, weight_col, bias_col, weight_col, bias_col, weight_row, weight_col, weight_col, weight_row, cache_spec, cache_spec)
    out_specs = (P("dp", None), cache_spec, cache_spec)

    def local_step(x_in, seq_lens, g_attn, g_mlp, w_q, b_q, w_k, b_k, w_v, b_v, w_o, w_gate, w_up, w_down, k_cache, v_cache):
        num_layers, rows, slots, kv_local, head = k_cache.shape
        kc = k_cache.reshape(num_layers, rows, slots, kv_local * head)
        vc = v_cache.reshape(num_layers, rows, slots, kv_local * head)
        act, x_res, outs = x_in, x_in, None
        cos_t = sin_t = jnp.zeros((8, head), F32)
        for layer in range(num_layers):
            last = layer == num_layers - 1
            attn, cos_t, sin_t, *outs = attention_call(
                layer, seq_lens, act, g_attn, b_q, b_k, b_v, cos_t, sin_t, w_q, w_k, w_v, kc, vc, outs)
            res = mlp_call(layer, last, attn, x_res, g_mlp, g_attn, w_o, w_gate, w_up, w_down)
            if last:
                x_out = res[0]
            else:
                act, x_res = res
        return x_out, outs[0].reshape(k_cache.shape), outs[1].reshape(v_cache.shape)

    return jax.shard_map(local_step, mesh=mesh, in_specs=in_specs, out_specs=out_specs, check_vma=False)
```

```python
import functools
import math

import jax
import jax.numpy as jnp
from jax import lax
from jax.experimental import pallas as pl
from jax.experimental.pallas import tpu as pltpu
from jax.sharding import PartitionSpec as P

ROPE_THETA = 1000000.0
EPS = 1e-6
MESH = pl.DeviceIdType.MESH
BF16 = jnp.bfloat16
F32 = jnp.float32
NCHUNK = 4
SEQ_BLOCK = 16
HBM = pl.BlockSpec(memory_space=pltpu.HBM)
VMEM = pl.BlockSpec(memory_space=pltpu.VMEM)
SMEM = pl.BlockSpec(memory_space=pltpu.SMEM)


def attention_kernel(layer, first, seq_ref, act_ref, g_ref, bq_ref, bk_ref, bv_ref, cos_in, sin_in, wq, wk, wv, kc, vc,
                     *rest):
    rest = list(rest)
    if not first:
        rest = rest[2:]
    attn_ref, cos_ref, sin_ref, k_out, v_out = rest[:5]
    h_s, w_s, kbuf, vbuf, qs, os, kn, vn, wsem, csem, osem = rest[5:]
    rows, width = act_ref.shape
    q_width = wq.shape[2]
    head = wk.shape[2]
    slots = kbuf.shape[1]
    heads = q_width // head
    kw = width // NCHUNK
    nblk = rows // SEQ_BLOCK

    def w_copies(c):
        ks = pl.ds(c * kw, kw)
        return [
            pltpu.make_async_copy(wq.at[layer, ks, :], w_s.at[ks, pl.ds(0, q_width)], wsem.at[c, 0]),
            pltpu.make_async_copy(wk.at[layer, ks, :], w_s.at[ks, pl.ds(q_width, head)], wsem.at[c, 1]),
            pltpu.make_async_copy(wv.at[layer, ks, :], w_s.at[ks, pl.ds(q_width + head, head)], wsem.at[c, 2]),
        ]

    def c_copies(i):
        bs = pl.ds(i * SEQ_BLOCK, SEQ_BLOCK)
        return [
            pltpu.make_async_copy(kc.at[layer, bs], kbuf.at[bs], csem.at[i, 0]),
            pltpu.make_async_copy(vc.at[layer, bs], vbuf.at[bs], csem.at[i, 1]),
        ]

    def o_copies(i):
        bs = pl.ds(i * SEQ_BLOCK, SEQ_BLOCK)
        return [
            pltpu.make_async_copy(kbuf.at[bs], k_out.at[layer, bs], osem.at[i, 0]),
            pltpu.make_async_copy(vbuf.at[bs], v_out.at[layer, bs], osem.at[i, 1]),
        ]

    for c in range(NCHUNK):
        for cp in w_copies(c):
            cp.start()
    for i in range(nblk):
        for cp in c_copies(i):
            cp.start()

    if first:
        def pos_row(b, carry):
            kn[pl.ds(b, 1), :] = jnp.full((1, head), seq_ref[b].astype(F32))
            return carry
        lax.fori_loop(0, rows, pos_row, 0, unroll=8)
        lane = lax.broadcasted_iota(jnp.int32, (rows, head), 1)
        half = head // 2
        freq = (lane % half).astype(F32)
        inv_freq = jnp.exp(freq[:8] * (-2.0 / head * math.log(ROPE_THETA)))
        angle = kn[...] * jnp.broadcast_to(inv_freq[:1], (rows, head))
        cos_ref[...] = jnp.cos(angle)
        sin_ref[...] = jnp.where(lane < half, -1.0, 1.0) * jnp.sin(angle)

        def norm_block(i, carry):
            rs = pl.ds(pl.multiple_of(i * 16, 16), 16)
            xv = act_ref[rs, :].astype(F32)
            ms = jnp.mean(xv * xv, axis=-1, keepdims=True)
            gain = g_ref[...].astype(F32)[layer:layer + 1, :]
            h_s[rs, :] = (xv * lax.rsqrt(ms + EPS) * gain).astype(BF16)
            return carry
        lax.fori_loop(0, rows // 16, norm_block, 0)
        h_src = h_s
    else:
        cos_ref[...] = cos_in[...]
        sin_ref[...] = sin_in[...]
        h_src = act_ref

    acc = None
    for c in range(NCHUNK):
        for cp in w_copies(c):
            cp.wait()
        part = jnp.dot(h_src[:, c * kw:(c + 1) * kw], w_s[c * kw:(c + 1) * kw, :], preferred_element_type=F32)
        acc = part if acc is None else acc + part
    cos_t = cos_ref[...]
    sin_t = sin_ref[...]

    def rope(vec):
        return vec * cos_t + pltpu.roll(vec, head // 2, 1) * sin_t

    bq = bq_ref[...].astype(F32)[layer:layer + 1, :]
    bk = bk_ref[...].astype(F32)[layer:layer + 1, :]
    bv = bv_ref[...].astype(F32)[layer:layer + 1, :]
    for j in range(heads):
        cols = slice(j * head, (j + 1) * head)
        qs[pl.ds(j, rows, stride=8), :] = rope(acc[:, cols] + bq[:, cols])
    kn[...] = rope(acc[:, q_width:q_width + head] + bk)
    vn[...] = acc[:, q_width + head:] + bv

    scale = head ** -0.5

    def block(i, carry):
        b0 = i * SEQ_BLOCK
        for cp in c_copies(i):
            cp.wait()
        tile_row = lax.broadcasted_iota(jnp.int32, (16, head), 0)
        lane = lax.broadcasted_iota(jnp.int32, (8, slots), 1)
        for j in range(SEQ_BLOCK):
            b = b0 + j
            pos = seq_ref[b]
            base = pl.multiple_of((pos // 16) * 16, 16)
            is_new = tile_row == pos - base
            for buf, new in ((kbuf, kn), (vbuf, vn)):
                old = buf[b, pl.ds(base, 16), :].astype(F32)
                row = jnp.broadcast_to(new[pl.ds(b, 1), :], (16, head))
                buf[b, pl.ds(base, 16), :] = jnp.where(is_new, row, old).astype(BF16)
        for cp in o_copies(i):
            cp.start()
        scores = []
        for j in range(0, SEQ_BLOCK, 2):
            b = b0 + j
            q_pair = qs[pl.ds(pl.multiple_of(b * 8, 16), 16), :].astype(BF16)
            k_pair = kbuf[pl.ds(b, 2)].reshape(2 * slots, head)
            sc = lax.dot_general(q_pair, k_pair, (((1,), (1,)), ((), ())), preferred_element_type=F32) * scale
            scores.append(jnp.where(lane <= seq_ref[b], sc[:8, :slots], -1e30))
            scores.append(jnp.where(lane <= seq_ref[b + 1], sc[8:, slots:], -1e30))
        sc = jnp.concatenate(scores, axis=0)
        e = jnp.exp(sc - jnp.max(sc, axis=-1, keepdims=True))
        pr = (e / jnp.sum(e, axis=-1, keepdims=True)).astype(BF16)
        for j in range(0, SEQ_BLOCK, 2):
            b = b0 + j
            v_pair = jnp.concatenate([vbuf[b], vbuf[b + 1]], axis=1)
            o_pair = jnp.dot(pr[j * 8:j * 8 + 16, :], v_pair, preferred_element_type=F32)
            os[pl.ds(pl.multiple_of(b * 8, 16), 8), :] = o_pair[:8, :head]
            os[pl.ds(pl.multiple_of(b * 8, 16) + 8, 8), :] = o_pair[8:, head:]
        return carry

    lax.fori_loop(0, nblk, block, 0)
    for j in range(heads):
        attn_ref[:, j * head:(j + 1) * head] = os[pl.ds(j, rows, stride=8), :].astype(BF16)
    for i in range(nblk):
        for cp in o_copies(i):
            cp.wait()


def attention_call(layer, seq_lens, act, g_attn, b_q, b_k, b_v, cos_t, sin_t, w_q, w_k, w_v, kc, vc, outs):
    first = outs is None
    rows, width = act.shape
    head = w_k.shape[2]
    q_width = w_q.shape[2]
    slots = kc.shape[2]
    nblk = rows // SEQ_BLOCK
    table = jax.ShapeDtypeStruct((rows, head), F32)
    operands = [seq_lens, act, g_attn, b_q, b_k, b_v, cos_t, sin_t, w_q, w_k, w_v, kc, vc]
    in_specs = [SMEM, VMEM, VMEM, VMEM, VMEM, VMEM, VMEM, VMEM, HBM, HBM, HBM, HBM, HBM]
    aliases = {}
    if not first:
        aliases = {len(operands): 3, len(operands) + 1: 4}
        operands += list(outs)
        in_specs += [HBM, HBM]
    return pl.pallas_call(
        functools.partial(attention_kernel, layer, first),
        out_shape=(jax.ShapeDtypeStruct((rows, q_width), BF16), table, table,
                   jax.ShapeDtypeStruct(kc.shape, BF16), jax.ShapeDtypeStruct(vc.shape, BF16)),
        in_specs=in_specs,
        out_specs=(VMEM, VMEM, VMEM, HBM, HBM),
        scratch_shapes=[
            pltpu.VMEM((rows, width), BF16),
            pltpu.VMEM((width, q_width + 2 * head), BF16),
            pltpu.VMEM((rows, slots, head), BF16),
            pltpu.VMEM((rows, slots, head), BF16),
            pltpu.VMEM((rows * 8, head), F32),
            pltpu.VMEM((rows * 8, head), F32),
            pltpu.VMEM((rows, head), F32),
            pltpu.VMEM((rows, head), F32),
            pltpu.SemaphoreType.DMA((NCHUNK, 3)),
            pltpu.SemaphoreType.DMA((nblk, 2)),
            pltpu.SemaphoreType.DMA((nblk, 2)),
        ],
        input_output_aliases=aliases,
        compiler_params=pltpu.CompilerParams(vmem_limit_bytes=62 << 20),
        name=f"attention_{layer}",
    )(*operands)


def mlp_kernel(layer, last, attn_ref, x_ref, gm_ref, gn_ref, wo, wg, wu, wd, *rest):
    n_out = 1 if last else 2
    outs = rest[:n_out]
    (wo_s, wg_s, wu_s, wd_s, part, r0, sa, sk, r1, sb, r2, xs, hbuf, gacc, uacc, act,
     wsem, xsem, ssem, rsem) = rest[n_out:]
    rows, width = hbuf.shape[1:]
    cw = width // NCHUNK
    unit = rows // 8
    me = lax.axis_index("tp")
    core = me % 2
    chip = me // 2
    flip_near = chip + 1 - 2 * (chip % 2)
    flip_far = 3 - chip
    bit_near = ((chip + 1) // 2) % 2
    bit_far = chip // 2
    dev_p = chip * 2 + 1 - core
    dev_a = ((1 - core) * flip_near + core * flip_far) * 2 + core
    dev_b = ((1 - core) * flip_far + core * flip_near) * 2 + core
    bit_a = (1 - core) * bit_near + core * bit_far
    bit_b = (1 - core) * bit_far + core * bit_near

    def row0(core_, a_, b_):
        return pl.multiple_of((core_ * 4 + a_ * 2 + b_) * unit, unit)

    own = row0(core, bit_a, bit_b)

    def wo_copy(c):
        return pltpu.make_async_copy(wo.at[layer, :, pl.ds(c * cw, cw)], wo_s.at[:, pl.ds(c * cw, cw)], wsem.at[0, c])

    def wg_copy(c):
        return pltpu.make_async_copy(wg.at[layer, pl.ds(c * cw, cw), :], wg_s.at[pl.ds(c * cw, cw), :], wsem.at[1, c])

    def wu_copy(c):
        return pltpu.make_async_copy(wu.at[layer, pl.ds(c * cw, cw), :], wu_s.at[pl.ds(c * cw, cw), :], wsem.at[2, c])

    def wd_copy(c):
        return pltpu.make_async_copy(wd.at[layer, :, pl.ds(c * cw, cw)], wd_s.at[:, pl.ds(c * cw, cw)], wsem.at[3, c])

    for c in range(NCHUNK):
        wo_copy(c).start()
    x_copy = None
    if x_ref.shape[0] != unit:
        x_copy = pltpu.make_async_copy(x_ref.at[pl.ds(own, unit), :], xs, xsem)
        x_copy.start()
    else:
        xs[...] = x_ref[...]

    barrier = pltpu.get_barrier_semaphore()
    for dev in (dev_p, dev_a, dev_b):
        pl.semaphore_signal(barrier, inc=1, device_id={"tp": dev}, device_id_type=MESH)
    pl.semaphore_wait(barrier, 3)

    def rcopy(ar, c, k, src, dst, dev):
        return pltpu.make_async_remote_copy(
            src_ref=src, dst_ref=dst, send_sem=ssem.at[ar, c, k], recv_sem=rsem.at[ar, c, k],
            device_id={"tp": dev}, device_id_type=MESH)

    def rs_p(ar, c):
        src = part.at[ar, c, pl.ds(pl.multiple_of((1 - core) * 4 * unit, unit), 4 * unit), :]
        return rcopy(ar, c, 0, src, r0.at[ar, c], dev_p)

    def rs_a(ar, c, k):
        return rcopy(ar, c, 1 + k, sa.at[ar, c, k], r1.at[ar, c, k], dev_a)

    def rs_b(ar, c):
        return rcopy(ar, c, 3, sb.at[ar, c], r2.at[ar, c], dev_b)

    def ag(ar, c, k, start, dev):
        blk = hbuf.at[ar, pl.ds(start, unit), pl.ds(c * cw, cw)]
        return rcopy(ar, c, 4 + k, blk, blk, dev)

    blk_b = row0(core, bit_a, 1 - bit_b)
    blk_a0 = row0(core, 1 - bit_a, bit_b)
    blk_a1 = row0(core, 1 - bit_a, 1 - bit_b)

    def ag_b(ar, c):
        return ag(ar, c, 0, own, dev_b)

    def ag_a(ar, c, k):
        return ag(ar, c, 1 + k, (own, blk_b)[k], dev_a)

    def ag_p(ar, c, k):
        return ag(ar, c, 3 + k, (own, blk_b, blk_a0, blk_a1)[k], dev_p)

    def reduce_scatter(ar, make_part):
        for c in range(NCHUNK):
            part[ar, c] = make_part(c).astype(BF16)
            rs_p(ar, c).start()
        for c in range(NCHUNK):
            rs_p(ar, c).wait_recv()

            def chip_sum(a_, b_):
                mine = part[ar, c, pl.ds(row0(core, a_, b_), unit), :].astype(F32)
                theirs = r0[ar, c, pl.ds(row0(0, a_, b_), unit), :].astype(F32)
                return mine + theirs

            sa[ar, c, 0] = chip_sum(1 - bit_a, 1 - bit_b).astype(BF16)
            rs_a(ar, c, 0).start()
            sa[ar, c, 1] = chip_sum(1 - bit_a, bit_b).astype(BF16)
            sk[c, 0] = chip_sum(bit_a, 1 - bit_b)
            sk[c, 1] = chip_sum(bit_a, bit_b)
        for c in range(NCHUNK):
            rs_a(ar, c, 1).start()
        for c in range(NCHUNK):
            rs_a(ar, c, 0).wait_recv()
            sb[ar, c] = (sk[c, 0] + r1[ar, c, 0].astype(F32)).astype(BF16)
            rs_b(ar, c).start()
        for c in range(NCHUNK):
            rs_a(ar, c, 1).wait_recv()
            rs_b(ar, c).wait_recv()
            delta = sk[c, 1] + r1[ar, c, 1].astype(F32) + r2[ar, c].astype(F32)
            cols = slice(c * cw, (c + 1) * cw)
            xs[:, cols] = (xs[:, cols].astype(F32) + delta).astype(BF16)

    def gather_start(ar):
        for c in range(NCHUNK):
            ag_b(ar, c).start()
            ag_a(ar, c, 0).start()
            ag_p(ar, c, 0).start()
        for c in range(NCHUNK):
            ag_b(ar, c).wait_recv()
            ag_a(ar, c, 1).start()
            ag_p(ar, c, 1).start()
        for c in range(NCHUNK):
            ag_a(ar, c, 0).wait_recv()
            ag_p(ar, c, 2).start()
        for c in range(NCHUNK):
            ag_a(ar, c, 1).wait_recv()
            ag_p(ar, c, 3).start()

    def gather_wait(ar, c):
        for k in range(4):
            ag_p(ar, c, k).wait_recv()

    def norm_own(gain):
        xv = xs[...].astype(F32)
        ms = jnp.mean(xv * xv, axis=-1, keepdims=True)
        return (xv * lax.rsqrt(ms + EPS) * gain).astype(BF16)

    def wo_part(c):
        wo_copy(c).wait()
        if c == NCHUNK - 1:
            for i in range(NCHUNK):
                wg_copy(i).start()
                wu_copy(i).start()
            for i in range(NCHUNK):
                wd_copy(i).start()
        return jnp.dot(attn_ref[...], wo_s[:, c * cw:(c + 1) * cw], preferred_element_type=F32)

    if x_copy is not None:
        x_copy.wait()
    reduce_scatter(0, wo_part)
    hbuf[0, pl.ds(own, unit), :] = norm_own(gm_ref[...].astype(F32)[layer:layer + 1, :])
    gather_start(0)
    for c in range(NCHUNK):
        gather_wait(0, c)
        wg_copy(c).wait()
        wu_copy(c).wait()
        ks = slice(c * cw, (c + 1) * cw)
        hc = hbuf[0, :, ks]
        gp = jnp.dot(hc, wg_s[ks, :], preferred_element_type=F32)
        up = jnp.dot(hc, wu_s[ks, :], preferred_element_type=F32)
        if c == 0:
            gacc[...] = gp
            uacc[...] = up
        elif c < NCHUNK - 1:
            gacc[...] += gp
            uacc[...] += up
        else:
            gate = gacc[...] + gp
            act[...] = (gate * jax.nn.sigmoid(gate) * (uacc[...] + up)).astype(BF16)

    def wd_part(c):
        wd_copy(c).wait()
        return jnp.dot(act[...], wd_s[:, c * cw:(c + 1) * cw], preferred_element_type=F32)

    reduce_scatter(1, wd_part)
    if last:
        hbuf[1, pl.ds(own, unit), :] = xs[...]
    else:
        hbuf[1, pl.ds(own, unit), :] = norm_own(gn_ref[...].astype(F32)[layer + 1:layer + 2, :])
        outs[1][...] = xs[...]
    gather_start(1)
    for c in range(NCHUNK):
        gather_wait(1, c)
        outs[0][:, c * cw:(c + 1) * cw] = hbuf[1, :, c * cw:(c + 1) * cw]
    for ar in range(2):
        for c in range(NCHUNK):
            rs_p(ar, c).wait_send()
            rs_b(ar, c).wait_send()
            ag_b(ar, c).wait_send()
            for k in range(2):
                rs_a(ar, c, k).wait_send()
                ag_a(ar, c, k).wait_send()
            for k in range(4):
                ag_p(ar, c, k).wait_send()


def mlp_call(layer, last, attn, x_res, g_mlp, g_attn, w_o, w_gate, w_up, w_down):
    rows = attn.shape[0]
    width = w_o.shape[2]
    inner = w_o.shape[1]
    ff = w_gate.shape[2]
    unit = rows // 8
    cw = width // NCHUNK
    full = jax.ShapeDtypeStruct((rows, width), BF16)
    out_shape = (full,) if last else (full, jax.ShapeDtypeStruct((unit, width), BF16))
    x_spec = VMEM if x_res.shape[0] == unit else HBM
    return pl.pallas_call(
        functools.partial(mlp_kernel, layer, last),
        out_shape=out_shape,
        in_specs=[VMEM, x_spec, VMEM, VMEM, HBM, HBM, HBM, HBM],
        out_specs=(VMEM,) * len(out_shape),
        scratch_shapes=[
            pltpu.VMEM((inner, width), BF16),
            pltpu.VMEM((width, ff), BF16),
            pltpu.VMEM((width, ff), BF16),
            pltpu.VMEM((ff, width), BF16),
            pltpu.VMEM((2, NCHUNK, rows, cw), BF16),
            pltpu.VMEM((2, NCHUNK, rows // 2, cw), BF16),
            pltpu.VMEM((2, NCHUNK, 2, unit, cw), BF16),
            pltpu.VMEM((NCHUNK, 2, unit, cw), F32),
            pltpu.VMEM((2, NCHUNK, 2, unit, cw), BF16),
            pltpu.VMEM((2, NCHUNK, unit, cw), BF16),
            pltpu.VMEM((2, NCHUNK, unit, cw), BF16),
            pltpu.VMEM((unit, width), BF16),
            pltpu.VMEM((2, rows, width), BF16),
            pltpu.VMEM((rows, ff), F32),
            pltpu.VMEM((rows, ff), F32),
            pltpu.VMEM((rows, ff), BF16),
            pltpu.SemaphoreType.DMA((4, NCHUNK)),
            pltpu.SemaphoreType.DMA,
            pltpu.SemaphoreType.DMA((2, NCHUNK, 11)),
            pltpu.SemaphoreType.DMA((2, NCHUNK, 11)),
        ],
        compiler_params=pltpu.CompilerParams(
            vmem_limit_bytes=62 << 20, collective_id=layer, has_side_effects=True),
        name=f"mlp_{layer}",
    )(attn, x_res, g_mlp, g_attn, w_o, w_gate, w_up, w_down)


def solution(mesh):
    assert mesh.shape["tp"] == 8
    weight_col = P(None, None, "tp")
    weight_row = P(None, "tp", None)
    bias_col = P(None, "tp")
    cache_spec = P(None, "dp", None, "tp", None)
    in_specs = (P("dp", None), P("dp"), P(None, None), P(None, None), weight_col, bias_col, weight_col, bias_col, weight_col, bias_col, weight_row, weight_col, weight_col, weight_row, cache_spec, cache_spec)
    out_specs = (P("dp", None), cache_spec, cache_spec)

    def local_step(x_in, seq_lens, g_attn, g_mlp, w_q, b_q, w_k, b_k, w_v, b_v, w_o, w_gate, w_up, w_down, k_cache, v_cache):
        num_layers, rows, slots, kv_local, head = k_cache.shape
        kc = k_cache.reshape(num_layers, rows, slots, kv_local * head)
        vc = v_cache.reshape(num_layers, rows, slots, kv_local * head)
        act, x_res, outs = x_in, x_in, None
        cos_t = sin_t = jnp.zeros((8, head), F32)
        for layer in range(num_layers):
            last = layer == num_layers - 1
            attn, cos_t, sin_t, *outs = attention_call(
                layer, seq_lens, act, g_attn, b_q, b_k, b_v, cos_t, sin_t, w_q, w_k, w_v, kc, vc, outs)
            res = mlp_call(layer, last, attn, x_res, g_mlp, g_attn, w_o, w_gate, w_up, w_down)
            if last:
                x_out = res[0]
            else:
                act, x_res = res
        return x_out, outs[0].reshape(k_cache.shape), outs[1].reshape(v_cache.shape)

    return jax.shard_map(local_step, mesh=mesh, in_specs=in_specs, out_specs=out_specs, check_vma=False)
```
